32 devices in a mesh: date: 4 (over y, x), path: 8 (over z, core).
Axes of the slice: x: 2, y: 2, z: 4, core: 2. Of those that a mesh axis runs over, the one named last changes fastest.
Arguments:
- factors: bfloat16 [32, 16, 32768], P('date', None, 'path'), may hold values from -10 to 10
- cashflows: bfloat16 [32, 64, 32768], P('date', None, 'path'), may hold values from -12 to 12
- frequency: bfloat16 [128, 16], replicated, may hold values from -1.5 to 1.5
- phases: float32 [128], replicated, may hold values from -3.140625 to 3.140625
- margin_lag: int32 [64], replicated, may hold values from 1 to 2
- thresholds: int32 [64], replicated, may hold values from 0 to 149
- transfer_min: int32 [64], replicated, may hold values from 0 to 59
Outputs:
- exposure: bfloat16 [32, 64, 32768], P('date', None, 'path')
- profile: float32 [32, 64], P('date')
The draws below stay inside these ranges and needn't reach their ends.
All inputs are finite; a program needn't handle non-finite values.
Results may differ from the reference program's by a relative error of at most 0.0058.
Values may be sent and summed in bfloat16 or wider, within the bound.
A program may use at most 128 MiB of HBM per device.

```python
import jax
import jax.numpy as jnp
from jax import lax

K = 128
NS = 64
R = 16
LAG_MAX = 2
DATES = 32
PATHS = 32768


def make_factors(key):
    scaled = jnp.clip(jax.random.normal(jax.random.fold_in(key, 11), (DATES, R, PATHS), jnp.float32), -5.0, 5.0)
    return scaled


def draw_factors(key, part):
    return make_factors(key).astype(jnp.bfloat16)


def draw_cashflows(key, part):
    scaled = make_factors(key)
    mixing = jax.random.normal(jax.random.fold_in(key, 13), (DATES, NS, R), jnp.float32) * (1.5 / R ** 0.5)
    signal = jnp.einsum('tnr,trp->tnp', mixing, scaled)
    noise_part = 0.4 * jax.random.normal(jax.random.fold_in(key, 14), (DATES, NS, PATHS), jnp.float32)
    flows = jnp.tanh(signal) + 0.3 * signal + noise_part
    return jnp.clip(flows, -12.0, 12.0).astype(jnp.bfloat16)


def touch_ends(drawn, key, least, top_value):
    shape = drawn.shape
    place = [jax.random.randint(jax.random.fold_in(key, axis), (), 0, shape[axis]) for axis in range(len(shape))]
    drawn = drawn.at[tuple(place)].set(least)
    longest = shape.index(max(shape))
    place[longest] = (place[longest] + 1) % shape[longest]
    return drawn.at[tuple(place)].set(top_value)


def bell_draw(stream_key, dims, scale, bound, held_as=jnp.bfloat16):
    drawn = scale * jax.random.normal(stream_key, dims, jnp.float32)
    return jnp.clip(drawn, min=-bound, max=bound).astype(held_as)


def setup_inputs(seed: int = 0) -> dict:
    streams_of = jax.random.split(jax.random.key(seed), 8)
    return {
        "factors": draw_factors(jax.random.fold_in(streams_of[7], 71), 0),
        "cashflows": draw_cashflows(jax.random.fold_in(streams_of[7], 71), 0),
        "frequency": bell_draw(streams_of[2], (K, R), R ** -0.5, 1.5),
        "phases": jnp.clip(jax.random.uniform(streams_of[3], (K,), jnp.float32, -3.140625, 3.140625), -3.140625, 3.140625),
        "margin_lag": touch_ends(jax.random.randint(streams_of[4], (NS,), 1, LAG_MAX + 1), jax.random.fold_in(streams_of[4], 1), 1, LAG_MAX).astype(jnp.int32),
        "thresholds": touch_ends(jax.random.randint(streams_of[5], (NS,), 0, 150), jax.random.fold_in(streams_of[5], 1), 0, 149).astype(jnp.int32),
        "transfer_min": touch_ends(jax.random.randint(streams_of[6], (NS,), 0, 60), jax.random.fold_in(streams_of[6], 1), 0, 59).astype(jnp.int32),
    }


ridge_weight = 0.05
root_two = 1.4142135623730951

def regress(gram_sum, right_sum, paths_all):
    system = gram_sum / paths_all + ridge_weight * jnp.eye(gram_sum.shape[-1], dtype=jnp.float32)
    factor = lax.linalg.cholesky(system)
    solved = lax.linalg.triangular_solve(factor, right_sum / paths_all, left_side=True, lower=True)
    solved = lax.linalg.triangular_solve(factor, solved, left_side=True, lower=True, transpose_a=True)
    return solved.astype(jnp.bfloat16)

def reference(factors, cashflows, frequency, phases, margin_lag, thresholds, transfer_min):
    paths_all = factors.shape[2]

    def one_date(inputs):
        state_now, flows_now = inputs
        angles = jnp.dot(frequency.astype(jnp.float32), state_now.astype(jnp.float32)) + phases[:, None]
        features = (root_two * jnp.cos(angles)).astype(jnp.bfloat16)
        gram_sum = jnp.dot(features.astype(jnp.float32), features.T.astype(jnp.float32), preferred_element_type=jnp.float32)
        right_sum = jnp.dot(features.astype(jnp.float32), flows_now.T.astype(jnp.float32), preferred_element_type=jnp.float32)
        coefficients = regress(gram_sum, right_sum, paths_all)
        return jnp.dot(coefficients.T.astype(jnp.float32), features.astype(jnp.float32), preferred_element_type=jnp.float32).astype(jnp.bfloat16)
    values = lax.map(one_date, (factors, cashflows))
    offset = (thresholds + transfer_min).astype(jnp.float32) / 100.0

    def expose(date_index):
        current = lax.dynamic_index_in_dim(values, date_index, 0, keepdims=False).astype(jnp.float32)
        lagged = jnp.zeros_like(current)
        for lag_value in range(1, LAG_MAX + 1):
            source = date_index - lag_value
            shifted = lax.dynamic_index_in_dim(values, jnp.maximum(source, 0).astype(jnp.int32), 0, keepdims=False).astype(jnp.float32)
            shifted = jnp.where(source >= 0, shifted, jnp.zeros_like(shifted))
            lagged = jnp.where((margin_lag == lag_value)[:, None], shifted, lagged)
        collateral = jnp.maximum(lagged - offset[:, None], 0.0)
        exposure = jnp.maximum(current - collateral, 0.0)
        return (exposure.astype(jnp.bfloat16), jnp.sum(exposure, axis=1) / paths_all)
    exposure, profile = lax.map(expose, jnp.arange(values.shape[0], dtype=jnp.int32))
    return (exposure, profile)
```

```python
import functools

import jax
import jax.numpy as jnp
from jax import lax
from jax.experimental import pallas as pl
from jax.experimental.pallas import tpu as pltpu
from jax.sharding import PartitionSpec as P

LAG_MAX = 2
MESH = pl.DeviceIdType.MESH
f32 = jnp.float32
bf16 = jnp.bfloat16

ridge_weight = 0.05
inverse_turn = 0.15915494309189535
root_two = 1.4142135623730951
half_wave = (1.6817899533136271, -8.29873762982186, 6.809195244612708, -2.0985399883857303)
newton_steps = 8
FEATURE_WIDTH = 512
VALUE_WIDTH = 512


def split(x, parts):
    out = []
    for _ in range(parts):
        piece = x.astype(bf16)
        out.append(piece)
        x = x - piece.astype(f32)
    return out


def contract(left, right):
    return lax.dot_general(left, right, (((1,), (0,)), ((), ())), preferred_element_type=f32)


def contract_last(left, right):
    return lax.dot_general(left, right, (((1,), (1,)), ((), ())), preferred_element_type=f32)


def product(left, right):
    if len(left) == 2:
        lh, lm = left
        rh, rm = right
        return contract(
            jnp.concatenate([lh, lm, lh, lm], axis=1), jnp.concatenate([rh, rh, rm, rm], axis=0)
        )
    lh, lm, ll = left
    rh, rm, rl = right
    return contract(
        jnp.concatenate([lh, lm, ll, lh, lm, lh], axis=1),
        jnp.concatenate([rh, rh, rh, rm, rm, rl], axis=0),
    )


def solve(system, right):
    size = system.shape[0]
    rows = lax.broadcasted_iota(jnp.int32, (size, size), 0)
    columns = lax.broadcasted_iota(jnp.int32, (size, size), 1)
    identity = jnp.where(rows == columns, 1.0, 0.0).astype(f32)
    top = 2.0 * size + ridge_weight
    least = 0.99 * ridge_weight / top
    scaled = system * (1.0 / top)
    inverse = None
    for step in range(newton_steps):
        weight = 2.0 / (1.0 + least)
        factor = 2.0 * identity - weight * scaled
        last = step == newton_steps - 1
        if inverse is None:
            inverse = (weight / top) * factor
            scaled = weight * product(split(scaled, 2), split(factor, 2))
        else:
            stack = inverse if last else jnp.concatenate([inverse, scaled], axis=0)
            stack = weight * product(split(stack, 2), split(factor, 2))
            inverse = stack[:size]
            scaled = None if last else stack[size:]
        least = 4.0 * least / (1.0 + least) ** 2
    inverse = split(inverse * (2.0 / (1.0 + least)), 3)
    found = product(split(right, 3), inverse)
    rest = right - product(split(found, 3), split(system, 3))
    return found + product(split(rest, 2), inverse[:2])


def as_column(row, width):
    return jnp.broadcast_to(row, (width, row.shape[1])).T


def kernel(
    axes,
    factors,
    cashflows,
    frequency,
    phases,
    margin_lag,
    thresholds,
    transfer_min,
    exposure,
    profile,
    state,
    flows,
    features,
    partial_sum,
    pair_part,
    pair_total,
    gathered,
    own_coefficients,
    coefficients,
    profile_own,
    profile_all,
    flows_sem,
    prior_send,
    prior_recv,
    pair_send,
    pair_recv,
    owner_send,
    owner_recv,
    coefficients_send,
    coefficients_recv,
    profile_send,
    profile_recv,
):
    slabs, group = axes
    dates, risk, paths = factors.shape
    terms = frequency.shape[1]
    sets = cashflows.shape[1]
    half = (terms + sets) // 2
    spread = group // dates
    paths_all = paths * group
    slab = lax.axis_index("date")
    me = lax.axis_index("path")
    partner = me + 1 - 2 * lax.rem(me, 2)
    side = lax.rem(me, 2)
    first = (2 * lax.div(me, 2)) // spread
    near = max(1, (2 * dates) // group)
    has_prior = slab > 0
    has_next = slab < slabs - 1

    def device(slab_index, path_index):
        return (slab_index, path_index)

    def date_at(step):
        return lax.rem(first + near + step, dates)

    def step_of(date):
        return lax.rem(date - first - near + 2 * dates, dates)

    barrier = pltpu.get_barrier_semaphore()

    def greet(j, carry):
        @pl.when(j != me)
        def _():
            pl.semaphore_signal(barrier, inc=1, device_id=device(slab, j), device_id_type=MESH)

        @pl.when(has_prior)
        def _():
            pl.semaphore_signal(barrier, inc=1, device_id=device(slab - 1, j), device_id_type=MESH)

        @pl.when(has_next)
        def _():
            pl.semaphore_signal(barrier, inc=1, device_id=device(slab + 1, j), device_id_type=MESH)

        return carry

    def flows_copy(step):
        return pltpu.make_async_copy(
            cashflows.at[date_at(step)], flows.at[step], flows_sem.at[step]
        )

    def load(step, carry):
        flows_copy(step).start()
        return carry

    lax.fori_loop(0, dates, load, 0)
    lax.fori_loop(0, group, greet, 0)

    turn = split(frequency[...].astype(f32).T * inverse_turn, 3)
    phase = split(as_column(phases[...] * inverse_turn, terms), 3)
    lane = lax.broadcasted_iota(jnp.int32, (terms, risk), 1)
    offset_part = jnp.zeros((terms, risk), f32)
    for i, piece in enumerate(phase):
        offset_part = jnp.where(lane == i, piece.astype(f32)[:, :risk], offset_part)
    wave_map = jnp.concatenate([piece.astype(f32) for piece in turn] + [offset_part], axis=1)
    wave_map = wave_map.astype(bf16)

    def featurize(source, date, slot, first_column):
        columns = pl.ds(first_column, FEATURE_WIDTH)
        now = source[date, :, columns]
        stacked = jnp.concatenate([now, now, now, jnp.ones(now.shape, bf16)], axis=0)
        turns = contract(wave_map, stacked)
        turns = turns - jnp.round(turns)
        square = turns * turns
        total = half_wave[-1]
        for term in half_wave[-2::-1]:
            total = total * square + term
        features[slot, :, columns] = (total * total - root_two).astype(bf16)

    def pair_copy(step):
        there = pl.ds(pl.multiple_of((1 - side) * half, 8), half)
        return pltpu.make_async_remote_copy(
            src_ref=partial_sum.at[step, there],
            dst_ref=pair_part.at[step],
            send_sem=pair_send.at[step],
            recv_sem=pair_recv.at[step],
            device_id=device(slab, partner),
            device_id_type=MESH,
        )

    def owner_copy(step, owner, slot):
        return pltpu.make_async_remote_copy(
            src_ref=pair_total.at[step],
            dst_ref=gathered.at[slot],
            send_sem=owner_send.at[step],
            recv_sem=owner_recv.at[slot],
            device_id=device(slab, owner),
            device_id_type=MESH,
        )

    def deliver(step):
        here = pl.ds(pl.multiple_of(side * half, 8), half)
        owner = date_at(step) * spread
        pair_copy(step).wait_recv()
        total = partial_sum[step, here] + pair_part[step]

        @pl.when(owner == me)
        def _():
            gathered[me] = total

        @pl.when(owner != me)
        def _():
            pair_total[step] = total
            owner_copy(step, owner, me).start()

    def prior_copy(target):
        return pltpu.make_async_remote_copy(
            src_ref=factors.at[pl.ds(dates - LAG_MAX, LAG_MAX)],
            dst_ref=state,
            send_sem=prior_send,
            recv_sem=prior_recv,
            device_id=device(target, me),
            device_id_type=MESH,
        )

    def gram(step):
        slot = LAG_MAX + step
        total = None
        for column in range(0, paths, FEATURE_WIDTH):
            featurize(factors, date_at(step), slot, column)
            columns = pl.ds(column, FEATURE_WIDTH)
            now = features[slot, :, columns]
            both = jnp.concatenate([now, flows[step, :, columns]], axis=0)
            part = contract_last(both, now)
            total = part if total is None else total + part
        partial_sum[step] = total

    def forward(step, carry):
        flows_copy(step).wait()
        gram(step)

        @pl.when(step == 0)
        def _():
            neighbours = (slab + slabs - 1) // slabs + (2 * slabs - 2 - slab) // slabs
            pl.semaphore_wait(barrier, group - 1 + group * neighbours)

        pair_copy(step).start()

        @pl.when(step > 0)
        def _():
            deliver(step - 1)

        return carry

    lax.fori_loop(0, dates, forward, 0)

    @pl.when(has_next)
    def _():
        prior_copy(slab + 1).start()

    deliver(dates - 1)

    @pl.when(has_prior)
    def _():
        prior_copy(slab).wait_recv()

        def prior(slot, carry):
            for column in range(0, paths, FEATURE_WIDTH):
                featurize(state, slot, slot, column)
            return carry

        lax.fori_loop(0, LAG_MAX, prior, 0)

    @pl.when(jnp.logical_not(has_prior))
    def _():
        features[pl.ds(0, LAG_MAX)] = jnp.zeros((LAG_MAX,) + features.shape[1:], bf16)
        coefficients[pl.ds(0, LAG_MAX)] = jnp.zeros((LAG_MAX, sets, terms), bf16)

    def coefficients_copy(target, j, slot, sem):
        return pltpu.make_async_remote_copy(
            src_ref=own_coefficients,
            dst_ref=coefficients.at[slot],
            send_sem=coefficients_send.at[sem],
            recv_sem=coefficients_recv.at[slot],
            device_id=device(target, j),
            device_id_type=MESH,
        )

    own = lax.div(me, spread)
    is_owner = lax.rem(me, spread) == 0
    tell_next = jnp.logical_and(
        jnp.logical_and(is_owner, has_next), own >= dates - LAG_MAX
    )

    @pl.when(is_owner)
    def _():
        def arrived(j, carry):
            @pl.when(j != me)
            def _():
                owner_copy(0, me, j).wait_recv()

            return carry

        lax.fori_loop(0, group, arrived, 0)
        upper = gathered[0]
        lower = gathered[1]
        for j in range(2, group, 2):
            upper = upper + gathered[j]
            lower = lower + gathered[j + 1]
        sums = jnp.concatenate([upper, lower], axis=0) * (1.0 / paths_all)
        rows = lax.broadcasted_iota(jnp.int32, (terms, terms), 0)
        columns = lax.broadcasted_iota(jnp.int32, (terms, terms), 1)
        system = sums[:terms] + jnp.where(rows == columns, ridge_weight, 0.0)
        answer = solve(system, sums[terms:]).astype(bf16)
        own_coefficients[...] = answer
        coefficients[LAG_MAX + own] = answer

        def tell(j, carry):
            @pl.when(j != me)
            def _():
                coefficients_copy(slab, j, LAG_MAX + own, j).start()

            return carry

        lax.fori_loop(0, group, tell, 0)

    @pl.when(tell_next)
    def _():
        def tell(j, carry):
            coefficients_copy(slab + 1, j, own - (dates - LAG_MAX), group + j).start()
            return carry

        lax.fori_loop(0, group, tell, 0)

    def arrived_coefficients(date, carry):
        @pl.when(date * spread != me)
        def _():
            coefficients_copy(slab, me, LAG_MAX + date, 0).wait_recv()

        return carry

    lax.fori_loop(0, dates, arrived_coefficients, 0)

    @pl.when(has_prior)
    def _():
        for i in range(LAG_MAX):
            coefficients_copy(slab, me, i, 0).wait_recv()

    lag = as_column(margin_lag[...].astype(f32), 128)
    offset = as_column((thresholds[...] + transfer_min[...]).astype(f32) / 100.0, 128)
    repeat = VALUE_WIDTH // 128
    lag = jnp.concatenate([lag] * repeat, axis=1)
    offset = jnp.concatenate([offset] * repeat, axis=1)

    def expose(block, totals):
        columns = pl.ds(pl.multiple_of(block * VALUE_WIDTH, VALUE_WIDTH), VALUE_WIDTH)
        earlier = []
        new_totals = []
        for date in range(-LAG_MAX, dates):
            slot = LAG_MAX + date if date < 0 else LAG_MAX + step_of(date)
            value = contract(coefficients[LAG_MAX + date], features[slot, :, columns])
            value = value.astype(bf16)
            if date >= 0:
                lagged = jnp.zeros(value.shape, f32)
                for lag_value in range(1, LAG_MAX + 1):
                    lagged = jnp.where(
                        lag == lag_value, earlier[-lag_value].astype(f32), lagged
                    )
                collateral = jnp.maximum(lagged - offset, 0.0)
                open_value = jnp.maximum(value.astype(f32) - collateral, 0.0)
                exposure[date, :, columns] = open_value.astype(bf16)
                total = totals[date]
                for i in range(repeat):
                    total = total + open_value[:, 128 * i : 128 * (i + 1)]
                new_totals.append(total)
            earlier.append(value)
        return tuple(new_totals)

    blocks = paths // VALUE_WIDTH
    totals = tuple(jnp.zeros((sets, 128), f32) for _ in range(dates))
    totals = lax.fori_loop(0, blocks, expose, totals)
    rows = [jnp.sum(total.T, axis=0, keepdims=True) for total in totals]
    profile_own[...] = jnp.concatenate(rows, axis=0)

    def profile_copy(j, slot):
        return pltpu.make_async_remote_copy(
            src_ref=profile_own,
            dst_ref=profile_all.at[slot],
            send_sem=profile_send.at[j],
            recv_sem=profile_recv.at[slot],
            device_id=device(slab, j),
            device_id_type=MESH,
        )

    def share(j, carry):
        @pl.when(j != me)
        def _():
            profile_copy(j, me).start()

        return carry

    lax.fori_loop(0, group, share, 0)
    profile_all[me] = profile_own[...]

    def received(j, carry):
        @pl.when(j != me)
        def _():
            profile_copy(0, j).wait_recv()

        return carry

    lax.fori_loop(0, group, received, 0)
    total = profile_all[0]
    for j in range(1, group):
        total = total + profile_all[j]
    profile[...] = total * (1.0 / paths_all)

    def sent(step, carry):
        pair_copy(step).wait_send()

        @pl.when(date_at(step) * spread != me)
        def _():
            owner_copy(step, me, me).wait_send()

        return carry

    lax.fori_loop(0, dates, sent, 0)

    def told(j, carry):
        @pl.when(j != me)
        def _():
            profile_copy(j, me).wait_send()

            @pl.when(is_owner)
            def _():
                coefficients_copy(slab, me, 0, j).wait_send()

        @pl.when(tell_next)
        def _():
            coefficients_copy(slab, me, 0, group + j).wait_send()

        return carry

    lax.fori_loop(0, group, told, 0)

    @pl.when(has_next)
    def _():
        prior_copy(slab).wait_send()


def local(axes, factors, cashflows, frequency, phases, margin_lag, thresholds, transfer_min):
    slabs, group = axes
    dates, risk, paths = factors.shape
    sets = cashflows.shape[1]
    terms = frequency.shape[0]
    half = (terms + sets) // 2
    anywhere = pl.BlockSpec(memory_space=pltpu.HBM)
    inside = pl.BlockSpec(memory_space=pltpu.VMEM)
    dma = pltpu.SemaphoreType.DMA
    return pl.pallas_call(
        functools.partial(kernel, axes),
        out_shape=(
            jax.ShapeDtypeStruct(cashflows.shape, bf16),
            jax.ShapeDtypeStruct((dates, sets), f32),
        ),
        in_specs=[inside, anywhere] + [inside] * 5,
        out_specs=(inside, inside),
        scratch_shapes=[
            pltpu.VMEM((LAG_MAX, risk, paths), bf16),
            pltpu.VMEM((dates, sets, paths), bf16),
            pltpu.VMEM((LAG_MAX + dates, terms, paths), bf16),
            pltpu.VMEM((dates, terms + sets, terms), f32),
            pltpu.VMEM((dates, half, terms), f32),
            pltpu.VMEM((dates, half, terms), f32),
            pltpu.VMEM((group, half, terms), f32),
            pltpu.VMEM((sets, terms), bf16),
            pltpu.VMEM((LAG_MAX + dates, sets, terms), bf16),
            pltpu.VMEM((dates, sets), f32),
            pltpu.VMEM((group, dates, sets), f32),
            dma((dates,)),
            dma,
            dma,
            dma((dates,)),
            dma((dates,)),
            dma((dates,)),
            dma((group,)),
            dma((2 * group,)),
            dma((LAG_MAX + dates,)),
            dma((group,)),
            dma((group,)),
        ],
        compiler_params=pltpu.CompilerParams(
            collective_id=0, has_side_effects=True, vmem_limit_bytes=48 * 1024 * 1024
        ),
    )(
        factors,
        cashflows,
        frequency.T,
        phases.reshape(1, terms),
        margin_lag.reshape(1, sets),
        thresholds.reshape(1, sets),
        transfer_min.reshape(1, sets),
    )


def solution(mesh):
    axes = (mesh.shape["date"], mesh.shape["path"])
    return jax.shard_map(
        functools.partial(local, axes),
        mesh=mesh,
        in_specs=(P("date", None, "path"), P("date", None, "path"), P(), P(), P(), P(), P()),
        out_specs=(P("date", None, "path"), P("date", None)),
        check_vma=False,
    )
```

```python
import functools

import jax
import jax.numpy as jnp
from jax import lax
from jax.experimental import pallas as pl
from jax.experimental.pallas import tpu as pltpu
from jax.sharding import PartitionSpec as P

LAG_MAX = 2
MESH = pl.DeviceIdType.MESH
f32 = jnp.float32
bf16 = jnp.bfloat16

ridge_weight = 0.05
inverse_turn = 0.15915494309189535
root_two = 1.4142135623730951
half_wave = (1.6817899533136271, -8.29873762982186, 6.809195244612708, -2.0985399883857303)
newton_steps = 8
FEATURE_WIDTH = 2048
VALUE_WIDTH = 1024
EXPOSE_WIDTH = 512
VMEM_LIMIT = 60751872


def split(x, parts):
    out = []
    for _ in range(parts):
        piece = x.astype(bf16)
        out.append(piece)
        x = x - piece.astype(f32)
    return out


def contract(left, right):
    return lax.dot_general(left, right, (((1,), (0,)), ((), ())), preferred_element_type=f32)


def contract_last(left, right):
    return lax.dot_general(left, right, (((1,), (1,)), ((), ())), preferred_element_type=f32)


def product(left, right):
    if len(left) == 2:
        lh, lm = left
        rh, rm = right
        return contract(
            jnp.concatenate([lh, lm, lh, lm], axis=1), jnp.concatenate([rh, rh, rm, rm], axis=0)
        )
    lh, lm, ll = left
    rh, rm, rl = right
    return contract(
        jnp.concatenate([lh, lm, ll, lh, lm, lh], axis=1),
        jnp.concatenate([rh, rh, rh, rm, rm, rl], axis=0),
    )


def solve(system, right):
    size = system.shape[0]
    rows = lax.broadcasted_iota(jnp.int32, (size, size), 0)
    columns = lax.broadcasted_iota(jnp.int32, (size, size), 1)
    identity = jnp.where(rows == columns, 1.0, 0.0).astype(f32)
    top = 2.0 * size + ridge_weight
    least = 0.99 * ridge_weight / top
    scaled = system * (1.0 / top)
    inverse = None
    for step in range(newton_steps):
        weight = 2.0 / (1.0 + least)
        factor = 2.0 * identity - weight * scaled
        last = step == newton_steps - 1
        if inverse is None:
            inverse = (weight / top) * factor
            scaled = weight * product(split(scaled, 2), split(factor, 2))
        else:
            stack = inverse if last else jnp.concatenate([inverse, scaled], axis=0)
            stack = weight * product(split(stack, 2), split(factor, 2))
            inverse = stack[:size]
            scaled = None if last else stack[size:]
        least = 4.0 * least / (1.0 + least) ** 2
    inverse = split(inverse * (2.0 / (1.0 + least)), 3)
    found = product(split(right, 3), inverse)
    rest = right - product(split(found, 3), split(system, 3))
    return found + product(split(rest, 2), inverse[:2])


def as_column(row, width):
    return jnp.broadcast_to(row, (width, row.shape[1])).T


def kernel(
    axes,
    factors_far,
    cashflows,
    frequency_far,
    phases_far,
    margin_lag_far,
    thresholds_far,
    transfer_min_far,
    exposure,
    profile,
    frequency,
    phases,
    margin_lag,
    thresholds,
    transfer_min,
    factors,
    state,
    flows,
    features,
    partial_sum,
    pair_part,
    pair_total,
    gathered,
    own_coefficients,
    coefficients,
    profile_own,
    profile_all,
    values,
    totals,
    small_sem,
    state_sem,
    flows_sem,
    prior_send,
    prior_recv,
    pair_send,
    pair_recv,
    owner_send,
    owner_recv,
    coefficients_send,
    coefficients_recv,
    profile_send,
    profile_recv,
):
    slabs, group = axes
    dates, risk, paths = factors_far.shape
    terms = frequency.shape[1]
    sets = cashflows.shape[1]
    half = (terms + sets) // 2
    spread = group // dates
    paths_all = paths * group
    slab = lax.axis_index("date")
    me = lax.axis_index("path")
    partner = me + 1 - 2 * lax.rem(me, 2)
    side = lax.rem(me, 2)
    first = (2 * lax.div(me, 2)) // spread
    near = max(1, (2 * dates) // group)
    has_prior = slab > 0
    has_next = slab < slabs - 1

    def device(slab_index, path_index):
        return (slab_index, path_index)

    def date_at(step):
        return lax.rem(first + near + step, dates)

    def step_of(date):
        return lax.rem(date - first - near + 2 * dates, dates)

    barrier = pltpu.get_barrier_semaphore()

    def greet(j, carry):
        @pl.when(j != me)
        def _():
            pl.semaphore_signal(barrier, inc=1, device_id=device(slab, j), device_id_type=MESH)

        @pl.when(has_prior)
        def _():
            pl.semaphore_signal(barrier, inc=1, device_id=device(slab - 1, j), device_id_type=MESH)

        @pl.when(has_next)
        def _():
            pl.semaphore_signal(barrier, inc=1, device_id=device(slab + 1, j), device_id_type=MESH)

        return carry

    def flows_copy(step):
        return pltpu.make_async_copy(
            cashflows.at[date_at(step)], flows.at[step], flows_sem.at[step]
        )

    def state_copy(step):
        return pltpu.make_async_copy(
            factors_far.at[date_at(step)], factors.at[step], state_sem.at[step]
        )

    small = [
        pltpu.make_async_copy(source, target, small_sem.at[i])
        for i, (source, target) in enumerate(
            (
                (frequency_far, frequency),
                (phases_far, phases),
                (margin_lag_far, margin_lag),
                (thresholds_far, thresholds),
                (transfer_min_far, transfer_min),
            )
        )
    ]
    for copy in small:
        copy.start()

    def load(step, carry):
        state_copy(step).start()
        flows_copy(step).start()
        return carry

    lax.fori_loop(0, dates, load, 0)
    lax.fori_loop(0, group, greet, 0)

    for copy in small:
        copy.wait()
    turn = split(frequency[...].astype(f32).T * inverse_turn, 3)
    phase = split(as_column(phases[...] * inverse_turn, terms), 3)
    lane = lax.broadcasted_iota(jnp.int32, (terms, risk), 1)
    offset_part = jnp.zeros((terms, risk), f32)
    for i, piece in enumerate(phase):
        offset_part = jnp.where(lane == i, piece.astype(f32)[:, :risk], offset_part)
    wave_map = jnp.concatenate([piece.astype(f32) for piece in turn] + [offset_part], axis=1)
    wave_map = wave_map.astype(bf16)

    def featurize(source, date, slot, first_column):
        columns = pl.ds(first_column, FEATURE_WIDTH)
        now = source[date, :, columns]
        stacked = jnp.concatenate([now, now, now, jnp.ones(now.shape, bf16)], axis=0)
        turns = contract(wave_map, stacked)
        turns = turns - jnp.round(turns)
        square = turns * turns
        total = half_wave[-1]
        for term in half_wave[-2::-1]:
            total = total * square + term
        features[slot, :, columns] = (total * total - root_two).astype(bf16)

    def pair_copy(step):
        there = pl.ds(pl.multiple_of((1 - side) * half, 8), half)
        return pltpu.make_async_remote_copy(
            src_ref=partial_sum.at[step, there],
            dst_ref=pair_part.at[step],
            send_sem=pair_send.at[step],
            recv_sem=pair_recv.at[step],
            device_id=device(slab, partner),
            device_id_type=MESH,
        )

    def owner_copy(step, owner, slot):
        return pltpu.make_async_remote_copy(
            src_ref=pair_total.at[step],
            dst_ref=gathered.at[slot],
            send_sem=owner_send.at[step],
            recv_sem=owner_recv.at[slot],
            device_id=device(slab, owner),
            device_id_type=MESH,
        )

    def deliver(step):
        here = pl.ds(pl.multiple_of(side * half, 8), half)
        owner = date_at(step) * spread
        pair_copy(step).wait_recv()
        total = partial_sum[step, here] + pair_part[step]

        @pl.when(owner == me)
        def _():
            gathered[me] = total

        @pl.when(owner != me)
        def _():
            pair_total[step] = total
            owner_copy(step, owner, me).start()

    def prior_copy(target):
        return pltpu.make_async_remote_copy(
            src_ref=factors_far.at[pl.ds(dates - LAG_MAX, LAG_MAX)],
            dst_ref=state,
            send_sem=prior_send,
            recv_sem=prior_recv,
            device_id=device(target, me),
            device_id_type=MESH,
        )

    def gram(step):
        slot = LAG_MAX + step
        total = None
        for column in range(0, paths, FEATURE_WIDTH):
            featurize(factors, step, slot, column)
            columns = pl.ds(column, FEATURE_WIDTH)
            now = features[slot, :, columns]
            both = jnp.concatenate([now, flows[step, :, columns]], axis=0)
            part = contract_last(both, now)
            total = part if total is None else total + part
        partial_sum[step] = total

    def forward(step, carry):
        state_copy(step).wait()
        flows_copy(step).wait()
        gram(step)

        @pl.when(step == 0)
        def _():
            neighbours = (slab + slabs - 1) // slabs + (2 * slabs - 2 - slab) // slabs
            pl.semaphore_wait(barrier, group - 1 + group * neighbours)

            @pl.when(has_next)
            def _():
                prior_copy(slab + 1).start()

        pair_copy(step).start()

        @pl.when(step > 0)
        def _():
            deliver(step - 1)

        return carry

    lax.fori_loop(0, dates, forward, 0)

    deliver(dates - 1)

    @pl.when(has_prior)
    def _():
        prior_copy(slab).wait_recv()

        def prior(slot, carry):
            for column in range(0, paths, FEATURE_WIDTH):
                featurize(state, slot, slot, column)
            return carry

        lax.fori_loop(0, LAG_MAX, prior, 0)

    def coefficients_copy(source, slab_index, path_index, slot, sem):
        return pltpu.make_async_remote_copy(
            src_ref=source,
            dst_ref=coefficients.at[slot],
            send_sem=coefficients_send.at[sem],
            recv_sem=coefficients_recv.at[slot],
            device_id=device(slab_index, path_index),
            device_id_type=MESH,
        )

    own = lax.div(me, spread)
    is_owner = lax.rem(me, spread) == 0
    chips = group // 2
    chip = lax.div(me, 2)
    relay = chips
    onward = chips + dates

    def evaluate(slot, feature_slot):
        for column in range(0, paths, VALUE_WIDTH):
            columns = pl.ds(column, VALUE_WIDTH)
            value = contract(coefficients[slot], features[feature_slot, :, columns])
            values[slot, :, columns] = value.astype(bf16)

    def pass_on(source, date):
        @pl.when(jnp.logical_and(has_next, date >= dates - LAG_MAX))
        def _():
            slot = date - (dates - LAG_MAX)
            coefficients_copy(source, slab + 1, me, slot, onward + slot).start()

    @pl.when(is_owner)
    def _():
        def arrived(j, carry):
            @pl.when(j != me)
            def _():
                owner_copy(0, me, j).wait_recv()

            return carry

        lax.fori_loop(0, group, arrived, 0)
        upper = gathered[0]
        lower = gathered[1]
        for j in range(2, group, 2):
            upper = upper + gathered[j]
            lower = lower + gathered[j + 1]
        sums = jnp.concatenate([upper, lower], axis=0) * (1.0 / paths_all)
        rows = lax.broadcasted_iota(jnp.int32, (terms, terms), 0)
        columns = lax.broadcasted_iota(jnp.int32, (terms, terms), 1)
        system = sums[:terms] + jnp.where(rows == columns, ridge_weight, 0.0)
        answer = solve(system, sums[terms:]).astype(bf16)
        own_coefficients[...] = answer
        coefficients[LAG_MAX + own] = answer

        def tell(distance, carry):
            for there in (chip + distance, chip - distance):

                @pl.when(jnp.logical_and(there >= 0, there < chips))
                def _():
                    coefficients_copy(
                        own_coefficients, slab, 2 * there + side, LAG_MAX + own, there
                    ).start()

            return carry

        lax.fori_loop(1, chips, tell, 0)
        coefficients_copy(own_coefficients, slab, partner, LAG_MAX + own, chip).start()
        pass_on(own_coefficients, own)
        evaluate(LAG_MAX + own, LAG_MAX + step_of(own))

    def visit(there, which):
        owner = 2 * there + which
        date = lax.div(owner, spread)
        slot = LAG_MAX + date

        @pl.when(jnp.logical_and(lax.rem(owner, spread) == 0, owner != me))
        def _():
            coefficients_copy(own_coefficients, slab, me, slot, 0).wait_recv()

            @pl.when(jnp.logical_and(which == side, there != chip))
            def _():
                coefficients_copy(
                    coefficients.at[slot], slab, partner, slot, relay + date
                ).start()

            pass_on(coefficients.at[slot], date)
            evaluate(slot, LAG_MAX + step_of(date))

    visit(chip, 1 - side)

    def collect(distance, carry):
        for there in (chip + distance, chip - distance):

            @pl.when(jnp.logical_and(there >= 0, there < chips))
            def _():
                def both(i, carry):
                    visit(there, lax.rem(side + i, 2))
                    return carry

                lax.fori_loop(0, 2, both, 0)

        return carry

    lax.fori_loop(1, chips, collect, 0)

    @pl.when(has_prior)
    def _():
        def prior(slot, carry):
            coefficients_copy(own_coefficients, slab, me, slot, 0).wait_recv()
            evaluate(slot, slot)
            return carry

        lax.fori_loop(0, LAG_MAX, prior, 0)

    @pl.when(jnp.logical_not(has_prior))
    def _():
        values[pl.ds(0, LAG_MAX)] = jnp.zeros((LAG_MAX, sets, paths), bf16)

    lag = as_column(margin_lag[...].astype(f32), 128)
    offset = as_column((thresholds[...] + transfer_min[...]).astype(f32) / 100.0, 128)
    repeat = EXPOSE_WIDTH // 128
    lag = jnp.concatenate([lag] * repeat, axis=1)
    offset = jnp.concatenate([offset] * repeat, axis=1)
    totals[...] = jnp.zeros(totals.shape, f32)

    def expose(block, carry):
        columns = pl.ds(pl.multiple_of(block * EXPOSE_WIDTH, EXPOSE_WIDTH), EXPOSE_WIDTH)
        earlier = [values[slot, :, columns].astype(f32) for slot in range(LAG_MAX)]
        for date in range(dates):
            value = values[LAG_MAX + date, :, columns].astype(f32)
            lagged = jnp.zeros(value.shape, f32)
            for lag_value in range(1, LAG_MAX + 1):
                lagged = jnp.where(lag == lag_value, earlier[-lag_value], lagged)
            collateral = jnp.maximum(lagged - offset, 0.0)
            open_value = jnp.maximum(value - collateral, 0.0)
            exposure[date, :, columns] = open_value.astype(bf16)
            total = open_value[:, :128]
            for i in range(1, repeat):
                total = total + open_value[:, 128 * i : 128 * (i + 1)]
            totals[date] = totals[date] + total
            earlier = earlier[1:] + [value]
        return carry

    lax.fori_loop(0, paths // EXPOSE_WIDTH, expose, 0)
    rows = [jnp.sum(totals[date].T, axis=0, keepdims=True) for date in range(dates)]
    profile_own[...] = jnp.concatenate(rows, axis=0)

    def profile_copy(j, slot):
        return pltpu.make_async_remote_copy(
            src_ref=profile_own,
            dst_ref=profile_all.at[slot],
            send_sem=profile_send.at[j],
            recv_sem=profile_recv.at[slot],
            device_id=device(slab, j),
            device_id_type=MESH,
        )

    def share(j, carry):
        @pl.when(j != me)
        def _():
            profile_copy(j, me).start()

        return carry

    lax.fori_loop(0, group, share, 0)
    profile_all[me] = profile_own[...]

    def received(j, carry):
        @pl.when(j != me)
        def _():
            profile_copy(0, j).wait_recv()

        return carry

    lax.fori_loop(0, group, received, 0)
    total = profile_all[0]
    for j in range(1, group):
        total = total + profile_all[j]
    profile[...] = total * (1.0 / paths_all)

    def sent(step, carry):
        pair_copy(step).wait_send()

        @pl.when(date_at(step) * spread != me)
        def _():
            owner_copy(step, me, me).wait_send()

        return carry

    lax.fori_loop(0, dates, sent, 0)

    def told(j, carry):
        @pl.when(j != me)
        def _():
            profile_copy(j, me).wait_send()

        return carry

    lax.fori_loop(0, group, told, 0)

    @pl.when(is_owner)
    def _():
        def told_chip(there, carry):
            coefficients_copy(own_coefficients, slab, me, 0, there).wait_send()
            return carry

        lax.fori_loop(0, chips, told_chip, 0)

    def relayed(date, carry):
        owner = date * spread

        @pl.when(jnp.logical_and(lax.rem(owner, 2) == side, lax.div(owner, 2) != chip))
        def _():
            coefficients_copy(own_coefficients, slab, me, 0, relay + date).wait_send()

        return carry

    lax.fori_loop(0, dates, relayed, 0)

    @pl.when(has_next)
    def _():
        for slot in range(LAG_MAX):
            coefficients_copy(own_coefficients, slab, me, 0, onward + slot).wait_send()

    @pl.when(has_next)
    def _():
        prior_copy(slab).wait_send()


def local(axes, factors, cashflows, frequency, phases, margin_lag, thresholds, transfer_min):
    slabs, group = axes
    dates, risk, paths = factors.shape
    sets = cashflows.shape[1]
    terms = frequency.shape[0]
    half = (terms + sets) // 2
    anywhere = pl.BlockSpec(memory_space=pltpu.HBM)
    inside = pl.BlockSpec(memory_space=pltpu.VMEM)
    dma = pltpu.SemaphoreType.DMA
    return pl.pallas_call(
        functools.partial(kernel, axes),
        out_shape=(
            pltpu.VMEM(cashflows.shape, bf16),
            jax.ShapeDtypeStruct((dates, sets), f32),
        ),
        in_specs=[anywhere] * 7,
        out_specs=(inside, inside),
        scratch_shapes=[
            pltpu.VMEM((risk, terms), bf16),
            pltpu.VMEM((1, terms), f32),
            pltpu.VMEM((1, sets), jnp.int32),
            pltpu.VMEM((1, sets), jnp.int32),
            pltpu.VMEM((1, sets), jnp.int32),
            pltpu.VMEM((dates, risk, paths), bf16),
            pltpu.VMEM((LAG_MAX, risk, paths), bf16),
            pltpu.VMEM((dates, sets, paths), bf16),
            pltpu.VMEM((LAG_MAX + dates, terms, paths), bf16),
            pltpu.VMEM((dates, terms + sets, terms), f32),
            pltpu.VMEM((dates, half, terms), f32),
            pltpu.VMEM((dates, half, terms), f32),
            pltpu.VMEM((group, half, terms), f32),
            pltpu.VMEM((sets, terms), bf16),
            pltpu.VMEM((LAG_MAX + dates, sets, terms), bf16),
            pltpu.VMEM((dates, sets), f32),
            pltpu.VMEM((group, dates, sets), f32),
            pltpu.VMEM((LAG_MAX + dates, sets, paths), bf16),
            pltpu.VMEM((dates, sets, 128), f32),
            dma((5,)),
            dma((dates,)),
            dma((dates,)),
            dma,
            dma,
            dma((dates,)),
            dma((dates,)),
            dma((dates,)),
            dma((group,)),
            dma((group // 2 + dates + LAG_MAX,)),
            dma((LAG_MAX + dates,)),
            dma((group,)),
            dma((group,)),
        ],
        compiler_params=pltpu.CompilerParams(
            collective_id=0, has_side_effects=True, vmem_limit_bytes=VMEM_LIMIT
        ),
    )(
        factors,
        cashflows,
        frequency.T,
        phases.reshape(1, terms),
        margin_lag.reshape(1, sets),
        thresholds.reshape(1, sets),
        transfer_min.reshape(1, sets),
    )


def solution(mesh):
    axes = (mesh.shape["date"], mesh.shape["path"])
    return jax.shard_map(
        functools.partial(local, axes),
        mesh=mesh,
        in_specs=(P("date", None, "path"), P("date", None, "path"), P(), P(), P(), P(), P()),
        out_specs=(P("date", None, "path"), P("date", None)),
        check_vma=False,
    )
```

```python
import functools

import jax
import jax.numpy as jnp
from jax import lax
from jax.experimental import pallas as pl
from jax.experimental.pallas import tpu as pltpu
from jax.sharding import PartitionSpec as P

LAG_MAX = 2
MESH = pl.DeviceIdType.MESH
f32 = jnp.float32
bf16 = jnp.bfloat16

ridge_weight = 0.05
inverse_turn = 0.15915494309189535
root_two = 1.4142135623730951
half_wave = (1.6817899533136271, -8.29873762982186, 6.809195244612708, -2.0985399883857303)
newton_steps = 8
FEATURE_WIDTH = 512
UNROLL = 2
VALUE_WIDTH = 1024
EXPOSE_WIDTH = 512
VMEM_LIMIT = 60751872


def split(x, parts):
    out = []
    for _ in range(parts):
        piece = x.astype(bf16)
        out.append(piece)
        x = x - piece.astype(f32)
    return out


def contract(left, right):
    return lax.dot_general(left, right, (((1,), (0,)), ((), ())), preferred_element_type=f32)


def contract_last(left, right):
    return lax.dot_general(left, right, (((1,), (1,)), ((), ())), preferred_element_type=f32)


def product(left, right):
    if len(left) == 2:
        lh, lm = left
        rh, rm = right
        return contract(
            jnp.concatenate([lh, lm, lh, lm], axis=1), jnp.concatenate([rh, rh, rm, rm], axis=0)
        )
    lh, lm, ll = left
    rh, rm, rl = right
    return contract(
        jnp.concatenate([lh, lm, ll, lh, lm, lh], axis=1),
        jnp.concatenate([rh, rh, rh, rm, rm, rl], axis=0),
    )


def solve(system, right):
    size = system.shape[0]
    rows = lax.broadcasted_iota(jnp.int32, (size, size), 0)
    columns = lax.broadcasted_iota(jnp.int32, (size, size), 1)
    identity = jnp.where(rows == columns, 1.0, 0.0).astype(f32)
    top = 2.0 * size + ridge_weight
    least = 0.99 * ridge_weight / top
    scaled = system * (1.0 / top)
    inverse = None
    for step in range(newton_steps):
        weight = 2.0 / (1.0 + least)
        factor = 2.0 * identity - weight * scaled
        last = step == newton_steps - 1
        if inverse is None:
            inverse = (weight / top) * factor
            scaled = weight * product(split(scaled, 2), split(factor, 2))
        else:
            stack = inverse if last else jnp.concatenate([inverse, scaled], axis=0)
            stack = weight * product(split(stack, 2), split(factor, 2))
            inverse = stack[:size]
            scaled = None if last else stack[size:]
        least = 4.0 * least / (1.0 + least) ** 2
    inverse = split(inverse * (2.0 / (1.0 + least)), 3)
    found = product(split(right, 3), inverse)
    rest = right - product(split(found, 3), split(system, 3))
    return found + product(split(rest, 2), inverse[:2])


def as_column(row, width):
    return jnp.broadcast_to(row, (width, row.shape[1])).T


def kernel(
    axes,
    factors_far,
    cashflows,
    frequency_far,
    phases_far,
    margin_lag_far,
    thresholds_far,
    transfer_min_far,
    exposure,
    profile,
    frequency,
    phases,
    margin_lag,
    thresholds,
    transfer_min,
    factors,
    state,
    flows,
    features,
    partial_sum,
    pair_part,
    pair_total,
    gathered,
    own_coefficients,
    coefficients,
    profile_own,
    profile_all,
    values,
    totals,
    small_sem,
    state_sem,
    flows_sem,
    prior_send,
    prior_recv,
    pair_send,
    pair_recv,
    owner_send,
    owner_recv,
    coefficients_send,
    coefficients_recv,
    profile_send,
    profile_recv,
):
    slabs, group = axes
    dates, risk, paths = factors_far.shape
    terms = frequency.shape[1]
    sets = cashflows.shape[1]
    half = (terms + sets) // 2
    spread = group // dates
    paths_all = paths * group
    slab = lax.axis_index("date")
    me = lax.axis_index("path")
    partner = me + 1 - 2 * lax.rem(me, 2)
    side = lax.rem(me, 2)
    first = (2 * lax.div(me, 2)) // spread
    near = max(1, (2 * dates) // group)
    has_prior = slab > 0
    has_next = slab < slabs - 1

    def device(slab_index, path_index):
        return (slab_index, path_index)

    places = dates // near
    place = first // near
    low = 2 * place < places

    def date_at(step):
        turn = step // near
        down = places - 1 - turn
        down = jnp.where(down > place, down, down - 1)
        up = jnp.where(turn < place, turn, turn + 1)
        there = jnp.where(low, down, up)
        there = jnp.where(turn == places - 1, place, there)
        return there * near + lax.rem(step, near)

    def step_of(date):
        there = date // near
        down = jnp.where(there > place, places - 1 - there, places - 2 - there)
        up = jnp.where(there < place, there, there - 1)
        turn = jnp.where(low, down, up)
        turn = jnp.where(there == place, places - 1, turn)
        return turn * near + lax.rem(date, near)

    barrier = pltpu.get_barrier_semaphore()

    def greet(j, carry):
        @pl.when(j != me)
        def _():
            pl.semaphore_signal(barrier, inc=1, device_id=device(slab, j), device_id_type=MESH)

        @pl.when(has_prior)
        def _():
            pl.semaphore_signal(barrier, inc=1, device_id=device(slab - 1, j), device_id_type=MESH)

        @pl.when(has_next)
        def _():
            pl.semaphore_signal(barrier, inc=1, device_id=device(slab + 1, j), device_id_type=MESH)

        return carry

    def flows_copy(step):
        return pltpu.make_async_copy(
            cashflows.at[date_at(step)], flows.at[step], flows_sem.at[step]
        )

    def state_copy(step):
        return pltpu.make_async_copy(
            factors_far.at[date_at(step)], factors.at[step], state_sem.at[step]
        )

    small = [
        pltpu.make_async_copy(source, target, small_sem.at[i])
        for i, (source, target) in enumerate(
            (
                (frequency_far, frequency),
                (phases_far, phases),
                (margin_lag_far, margin_lag),
                (thresholds_far, thresholds),
                (transfer_min_far, transfer_min),
            )
        )
    ]
    for copy in small:
        copy.start()

    def load(step):
        state_copy(step).start()
        flows_copy(step).start()

    for step in range(min(2 * UNROLL, dates)):
        load(step)
    lax.fori_loop(0, group, greet, 0)

    for copy in small:
        copy.wait()
    turn = split(frequency[...].astype(f32).T * inverse_turn, 3)
    phase = split(as_column(phases[...] * inverse_turn, terms), 3)
    lane = lax.broadcasted_iota(jnp.int32, (terms, risk), 1)
    offset_part = jnp.zeros((terms, risk), f32)
    for i, piece in enumerate(phase):
        offset_part = jnp.where(lane == i, piece.astype(f32)[:, :risk], offset_part)
    wave_map = jnp.concatenate([piece.astype(f32) for piece in turn] + [offset_part], axis=1)
    wave_map = wave_map.astype(bf16)

    def turns_of(source, date, first_column):
        now = source[date, :, pl.ds(first_column, FEATURE_WIDTH)]
        stacked = jnp.concatenate([now, now, now, jnp.ones(now.shape, bf16)], axis=0)
        return contract(wave_map, stacked)

    def wave_of(turns):
        turns = turns - jnp.round(turns)
        square = turns * turns
        total = half_wave[-1]
        for term in half_wave[-2::-1]:
            total = total * square + term
        return (total * total - root_two).astype(bf16)

    def pair_copy(step):
        there = pl.ds(pl.multiple_of((1 - side) * half, 8), half)
        return pltpu.make_async_remote_copy(
            src_ref=partial_sum.at[step, there],
            dst_ref=pair_part.at[step],
            send_sem=pair_send.at[step],
            recv_sem=pair_recv.at[step],
            device_id=device(slab, partner),
            device_id_type=MESH,
        )

    def owner_copy(step, owner, slot):
        return pltpu.make_async_remote_copy(
            src_ref=pair_total.at[step],
            dst_ref=gathered.at[slot],
            send_sem=owner_send.at[step],
            recv_sem=owner_recv.at[slot],
            device_id=device(slab, owner),
            device_id_type=MESH,
        )

    def pair_sum(step):
        here = pl.ds(pl.multiple_of(side * half, 8), half)
        pair_copy(step).wait_recv()
        return partial_sum[step, here] + pair_part[step]

    def deliver(step):
        pair_total[step] = pair_sum(step)
        owner_copy(step, date_at(step) * spread, me).start()

    def deliver_or_keep(step):
        owner = date_at(step) * spread
        total = pair_sum(step)

        @pl.when(owner == me)
        def _():
            gathered[me] = total

        @pl.when(owner != me)
        def _():
            pair_total[step] = total
            owner_copy(step, owner, me).start()

    def prior_copy(target):
        return pltpu.make_async_remote_copy(
            src_ref=factors_far.at[pl.ds(dates - LAG_MAX, LAG_MAX)],
            dst_ref=state,
            send_sem=prior_send,
            recv_sem=prior_recv,
            device_id=device(target, me),
            device_id_type=MESH,
        )

    def gram(steps, done):
        blocks = [(i, c) for i in range(len(steps)) for c in range(0, paths, FEATURE_WIDTH)]
        sums = [None] * len(steps)

        def accumulate(block, now):
            i, column = block
            flow = flows[steps[i], :, pl.ds(column, FEATURE_WIDTH)]
            part = contract_last(jnp.concatenate([now, flow], axis=0), now)
            sums[i] = part if sums[i] is None else sums[i] + part
            if column + FEATURE_WIDTH == paths:
                partial_sum[steps[i]] = sums[i]
                done(i)

        turns = turns_of(factors, steps[0], 0)
        before = None
        for n, (i, column) in enumerate(blocks):
            following = None
            if n + 1 < len(blocks):
                following = turns_of(factors, steps[blocks[n + 1][0]], blocks[n + 1][1])
            if before is not None:
                accumulate(blocks[n - 1], before)
            before = wave_of(turns)
            features[LAG_MAX + steps[i], :, pl.ds(column, FEATURE_WIDTH)] = before
            turns = following
        accumulate(blocks[-1], before)

    def ready(step):
        state_copy(step).wait()
        flows_copy(step).wait()

    def greeted():
        neighbours = (slab + slabs - 1) // slabs + (2 * slabs - 2 - slab) // slabs
        pl.semaphore_wait(barrier, group - 1 + group * neighbours)
        pair_copy(0).start()

        @pl.when(has_next)
        def _():
            prior_copy(slab + 1).start()

    ready(0)
    gram([0], lambda i: greeted())
    for step in range(1, UNROLL):
        ready(step)
        gram([step], lambda i: pair_copy(step).start())

    def forward(turn, carry):
        steps = [UNROLL * turn + i for i in range(UNROLL)]

        @pl.when(turn < dates // UNROLL - 1)
        def _():
            for step in steps:
                load(step + UNROLL)

        for step in steps:
            ready(step)
        deliver(steps[0] - UNROLL)

        def done(i):
            pair_copy(steps[i]).start()
            if i + 1 < UNROLL:
                deliver(steps[i + 1] - UNROLL)

        gram(steps, done)
        return carry

    lax.fori_loop(1, dates // UNROLL, forward, 0)

    for step in range(dates - UNROLL, dates):
        deliver_or_keep(step)

    @pl.when(has_prior)
    def _():
        prior_copy(slab).wait_recv()

        def prior(slot, carry):
            for column in range(0, paths, FEATURE_WIDTH):
                waves = wave_of(turns_of(state, slot, column))
                features[slot, :, pl.ds(column, FEATURE_WIDTH)] = waves
            return carry

        lax.fori_loop(0, LAG_MAX, prior, 0)

    def coefficients_copy(source, slab_index, path_index, slot, sem):
        return pltpu.make_async_remote_copy(
            src_ref=source,
            dst_ref=coefficients.at[slot],
            send_sem=coefficients_send.at[sem],
            recv_sem=coefficients_recv.at[slot],
            device_id=device(slab_index, path_index),
            device_id_type=MESH,
        )

    own = lax.div(me, spread)
    is_owner = lax.rem(me, spread) == 0
    chips = group // 2
    chip = lax.div(me, 2)
    relay = chips
    onward = chips + dates

    def evaluate(slot, feature_slot):
        for column in range(0, paths, VALUE_WIDTH):
            columns = pl.ds(column, VALUE_WIDTH)
            value = contract(coefficients[slot], features[feature_slot, :, columns])
            values[slot, :, columns] = value.astype(bf16)

    def pass_on(source, date):
        @pl.when(jnp.logical_and(has_next, date >= dates - LAG_MAX))
        def _():
            slot = date - (dates - LAG_MAX)
            coefficients_copy(source, slab + 1, me, slot, onward + slot).start()

    @pl.when(is_owner)
    def _():
        def arrived(j, carry):
            @pl.when(j != me)
            def _():
                owner_copy(0, me, j).wait_recv()

            return carry

        lax.fori_loop(0, group, arrived, 0)
        upper = gathered[0]
        lower = gathered[1]
        for j in range(2, group, 2):
            upper = upper + gathered[j]
            lower = lower + gathered[j + 1]
        sums = jnp.concatenate([upper, lower], axis=0) * (1.0 / paths_all)
        rows = lax.broadcasted_iota(jnp.int32, (terms, terms), 0)
        columns = lax.broadcasted_iota(jnp.int32, (terms, terms), 1)
        system = sums[:terms] + jnp.where(rows == columns, ridge_weight, 0.0)
        answer = solve(system, sums[terms:]).astype(bf16)
        own_coefficients[...] = answer
        coefficients[LAG_MAX + own] = answer

        def tell(distance, carry):
            for there in (chip + distance, chip - distance):

                @pl.when(jnp.logical_and(there >= 0, there < chips))
                def _():
                    coefficients_copy(
                        own_coefficients, slab, 2 * there + side, LAG_MAX + own, there
                    ).start()

            return carry

        lax.fori_loop(1, chips, tell, 0)
        coefficients_copy(own_coefficients, slab, partner, LAG_MAX + own, chip).start()
        pass_on(own_coefficients, own)
        evaluate(LAG_MAX + own, LAG_MAX + step_of(own))

    def visit(there, which):
        owner = 2 * there + which
        date = lax.div(owner, spread)
        slot = LAG_MAX + date

        @pl.when(jnp.logical_and(lax.rem(owner, spread) == 0, owner != me))
        def _():
            coefficients_copy(own_coefficients, slab, me, slot, 0).wait_recv()

            @pl.when(jnp.logical_and(which == side, there != chip))
            def _():
                coefficients_copy(
                    coefficients.at[slot], slab, partner, slot, relay + date
                ).start()

            pass_on(coefficients.at[slot], date)
            evaluate(slot, LAG_MAX + step_of(date))

    visit(chip, 1 - side)

    def collect(turn, carry):
        distance = 1 + lax.rem(turn, chips - 1)
        which = lax.rem(side + turn // (chips - 1), 2)

        for there in (chip + distance, chip - distance):

            @pl.when(jnp.logical_and(there >= 0, there < chips))
            def _():
                visit(there, which)

        return carry

    lax.fori_loop(0, 2 * (chips - 1), collect, 0)

    lag = as_column(margin_lag[...].astype(f32), 128)
    offset = as_column((thresholds[...] + transfer_min[...]).astype(f32) / 100.0, 128)
    repeat = EXPOSE_WIDTH // 128
    lag = jnp.concatenate([lag] * repeat, axis=1)
    offset = jnp.concatenate([offset] * repeat, axis=1)
    totals[...] = jnp.zeros(totals.shape, f32)

    def expose(first_date, end_date):
        def body(block, carry):
            start = pl.multiple_of(block * EXPOSE_WIDTH, EXPOSE_WIDTH)
            columns = pl.ds(start, EXPOSE_WIDTH)
            earlier = [
                values[first_date + slot, :, columns].astype(f32) for slot in range(LAG_MAX)
            ]
            for date in range(first_date, end_date):
                value = values[LAG_MAX + date, :, columns].astype(f32)
                lagged = jnp.zeros(value.shape, f32)
                for lag_value in range(1, LAG_MAX + 1):
                    lagged = jnp.where(lag == lag_value, earlier[-lag_value], lagged)
                collateral = jnp.maximum(lagged - offset, 0.0)
                open_value = jnp.maximum(value - collateral, 0.0)
                exposure[date, :, columns] = open_value.astype(bf16)
                total = open_value[:, :128]
                for i in range(1, repeat):
                    total = total + open_value[:, 128 * i : 128 * (i + 1)]
                totals[date] = totals[date] + total
                earlier = earlier[1:] + [value]
            return carry

        lax.fori_loop(0, paths // EXPOSE_WIDTH, body, 0)

    expose(LAG_MAX, dates)

    @pl.when(has_prior)
    def _():
        def prior(slot, carry):
            coefficients_copy(own_coefficients, slab, me, slot, 0).wait_recv()
            evaluate(slot, slot)
            return carry

        lax.fori_loop(0, LAG_MAX, prior, 0)

    @pl.when(jnp.logical_not(has_prior))
    def _():
        values[pl.ds(0, LAG_MAX)] = jnp.zeros((LAG_MAX, sets, paths), bf16)

    expose(0, LAG_MAX)
    rows = [jnp.sum(totals[date].T, axis=0, keepdims=True) for date in range(dates)]
    profile_own[...] = jnp.concatenate(rows, axis=0)

    def profile_copy(j, slot):
        return pltpu.make_async_remote_copy(
            src_ref=profile_own,
            dst_ref=profile_all.at[slot],
            send_sem=profile_send.at[j],
            recv_sem=profile_recv.at[slot],
            device_id=device(slab, j),
            device_id_type=MESH,
        )

    def share(j, carry):
        @pl.when(j != me)
        def _():
            profile_copy(j, me).start()

        return carry

    lax.fori_loop(0, group, share, 0)
    profile_all[me] = profile_own[...]

    def received(j, carry):
        @pl.when(j != me)
        def _():
            profile_copy(0, j).wait_recv()

        return carry

    lax.fori_loop(0, group, received, 0)
    total = profile_all[0]
    for j in range(1, group):
        total = total + profile_all[j]
    profile[...] = total * (1.0 / paths_all)

    def sent(step, carry):
        pair_copy(step).wait_send()

        @pl.when(date_at(step) * spread != me)
        def _():
            owner_copy(step, me, me).wait_send()

        return carry

    lax.fori_loop(0, dates, sent, 0)

    def told(j, carry):
        @pl.when(j != me)
        def _():
            profile_copy(j, me).wait_send()

        return carry

    lax.fori_loop(0, group, told, 0)

    @pl.when(is_owner)
    def _():
        def told_chip(there, carry):
            coefficients_copy(own_coefficients, slab, me, 0, there).wait_send()
            return carry

        lax.fori_loop(0, chips, told_chip, 0)

    def relayed(date, carry):
        owner = date * spread

        @pl.when(jnp.logical_and(lax.rem(owner, 2) == side, lax.div(owner, 2) != chip))
        def _():
            coefficients_copy(own_coefficients, slab, me, 0, relay + date).wait_send()

        return carry

    lax.fori_loop(0, dates, relayed, 0)

    @pl.when(has_next)
    def _():
        for slot in range(LAG_MAX):
            coefficients_copy(own_coefficients, slab, me, 0, onward + slot).wait_send()

    @pl.when(has_next)
    def _():
        prior_copy(slab).wait_send()


def local(axes, factors, cashflows, frequency, phases, margin_lag, thresholds, transfer_min):
    slabs, group = axes
    dates, risk, paths = factors.shape
    sets = cashflows.shape[1]
    terms = frequency.shape[0]
    half = (terms + sets) // 2
    anywhere = pl.BlockSpec(memory_space=pltpu.HBM)
    inside = pl.BlockSpec(memory_space=pltpu.VMEM)
    dma = pltpu.SemaphoreType.DMA
    return pl.pallas_call(
        functools.partial(kernel, axes),
        out_shape=(
            pltpu.VMEM(cashflows.shape, bf16),
            jax.ShapeDtypeStruct((dates, sets), f32),
        ),
        in_specs=[anywhere] * 7,
        out_specs=(inside, inside),
        scratch_shapes=[
            pltpu.VMEM((risk, terms), bf16),
            pltpu.VMEM((1, terms), f32),
            pltpu.VMEM((1, sets), jnp.int32),
            pltpu.VMEM((1, sets), jnp.int32),
            pltpu.VMEM((1, sets), jnp.int32),
            pltpu.VMEM((dates, risk, paths), bf16),
            pltpu.VMEM((LAG_MAX, risk, paths), bf16),
            pltpu.VMEM((dates, sets, paths), bf16),
            pltpu.VMEM((LAG_MAX + dates, terms, paths), bf16),
            pltpu.VMEM((dates, terms + sets, terms), f32),
            pltpu.VMEM((dates, half, terms), f32),
            pltpu.VMEM((dates, half, terms), f32),
            pltpu.VMEM((group, half, terms), f32),
            pltpu.VMEM((sets, terms), bf16),
            pltpu.VMEM((LAG_MAX + dates, sets, terms), bf16),
            pltpu.VMEM((dates, sets), f32),
            pltpu.VMEM((group, dates, sets), f32),
            pltpu.VMEM((LAG_MAX + dates, sets, paths), bf16),
            pltpu.VMEM((dates, sets, 128), f32),
            dma((5,)),
            dma((dates,)),
            dma((dates,)),
            dma,
            dma,
            dma((dates,)),
            dma((dates,)),
            dma((dates,)),
            dma((group,)),
            dma((group // 2 + dates + LAG_MAX,)),
            dma((LAG_MAX + dates,)),
            dma((group,)),
            dma((group,)),
        ],
        compiler_params=pltpu.CompilerParams(
            collective_id=0, has_side_effects=True, vmem_limit_bytes=VMEM_LIMIT
        ),
    )(
        factors,
        cashflows,
        frequency.T,
        phases.reshape(1, terms),
        margin_lag.reshape(1, sets),
        thresholds.reshape(1, sets),
        transfer_min.reshape(1, sets),
    )


def solution(mesh):
    axes = (mesh.shape["date"], mesh.shape["path"])
    return jax.shard_map(
        functools.partial(local, axes),
        mesh=mesh,
        in_specs=(P("date", None, "path"), P("date", None, "path"), P(), P(), P(), P(), P()),
        out_specs=(P("date", None, "path"), P("date", None)),
        check_vma=False,
    )
```

```python
import functools

import jax
import jax.numpy as jnp
from jax import lax
from jax.experimental import pallas as pl
from jax.experimental.pallas import tpu as pltpu
from jax.sharding import PartitionSpec as P

LAG_MAX = 2
MESH = pl.DeviceIdType.MESH
f32 = jnp.float32
bf16 = jnp.bfloat16

ridge_weight = 0.05
inverse_turn = 0.15915494309189535
root_two = 1.4142135623730951
half_wave = (1.6817899533136271, -8.29873762982186, 6.809195244612708, -2.0985399883857303)
newton_steps = 8
FEATURE_WIDTH = 512
UNROLL = 2
VALUE_WIDTH = 1024
EXPOSE_WIDTH = 512
VMEM_LIMIT = 60751872


def split(x, parts):
    out = []
    for _ in range(parts):
        piece = x.astype(bf16)
        out.append(piece)
        x = x - piece.astype(f32)
    return out


def contract(left, right):
    return lax.dot_general(left, right, (((1,), (0,)), ((), ())), preferred_element_type=f32)


def contract_last(left, right):
    return lax.dot_general(left, right, (((1,), (1,)), ((), ())), preferred_element_type=f32)


def product(left, right):
    if len(left) == 2:
        lh, lm = left
        rh, rm = right
        return contract(
            jnp.concatenate([lh, lm, lh, lm], axis=1), jnp.concatenate([rh, rh, rm, rm], axis=0)
        )
    lh, lm, ll = left
    rh, rm, rl = right
    return contract(
        jnp.concatenate([lh, lm, ll, lh, lm, lh], axis=1),
        jnp.concatenate([rh, rh, rh, rm, rm, rl], axis=0),
    )


def solve(system, right):
    size = system.shape[0]
    rows = lax.broadcasted_iota(jnp.int32, (size, size), 0)
    columns = lax.broadcasted_iota(jnp.int32, (size, size), 1)
    identity = jnp.where(rows == columns, 1.0, 0.0).astype(f32)
    top = 2.0 * size + ridge_weight
    least = 0.99 * ridge_weight / top
    scaled = system * (1.0 / top)
    inverse = None
    for step in range(newton_steps):
        weight = 2.0 / (1.0 + least)
        factor = 2.0 * identity - weight * scaled
        last = step == newton_steps - 1
        if inverse is None:
            inverse = (weight / top) * factor
            scaled = weight * product(split(scaled, 2), split(factor, 2))
        else:
            stack = inverse if last else jnp.concatenate([inverse, scaled], axis=0)
            stack = weight * product(split(stack, 2), split(factor, 2))
            inverse = stack[:size]
            scaled = None if last else stack[size:]
        least = 4.0 * least / (1.0 + least) ** 2
    inverse = split(inverse * (2.0 / (1.0 + least)), 3)
    found = product(split(right, 3), inverse)
    rest = right - product(split(found, 3), split(system, 3))
    return found + product(split(rest, 2), inverse[:2])


def as_column(row, width):
    return jnp.broadcast_to(row, (width, row.shape[1])).T


def kernel(
    axes,
    factors_far,
    cashflows,
    frequency_far,
    phases_far,
    margin_lag_far,
    thresholds_far,
    transfer_min_far,
    exposure,
    profile,
    frequency,
    phases,
    margin_lag,
    thresholds,
    transfer_min,
    factors,
    state,
    flows,
    features,
    partial_sum,
    pair_part,
    pair_total,
    gathered,
    own_coefficients,
    coefficients,
    profile_own,
    profile_all,
    values,
    totals,
    lag_column,
    offset_column,
    small_sem,
    state_sem,
    flows_sem,
    prior_send,
    prior_recv,
    pair_send,
    pair_recv,
    owner_send,
    owner_recv,
    coefficients_send,
    coefficients_recv,
    profile_send,
    profile_recv,
):
    slabs, group = axes
    dates, risk, paths = factors_far.shape
    terms = frequency.shape[1]
    sets = cashflows.shape[1]
    half = (terms + sets) // 2
    spread = group // dates
    paths_all = paths * group
    slab = lax.axis_index("date")
    me = lax.axis_index("path")
    partner = me + 1 - 2 * lax.rem(me, 2)
    side = lax.rem(me, 2)
    first = (2 * lax.div(me, 2)) // spread
    near = max(1, (2 * dates) // group)
    has_prior = slab > 0
    has_next = slab < slabs - 1

    def device(slab_index, path_index):
        return (slab_index, path_index)

    places = dates // near
    place = first // near
    low = 2 * place < places

    def date_at(step):
        turn = step // near
        down = places - 1 - turn
        down = jnp.where(down > place, down, down - 1)
        up = jnp.where(turn < place, turn, turn + 1)
        there = jnp.where(low, down, up)
        there = jnp.where(turn == places - 1, place, there)
        return there * near + lax.rem(step, near)

    def step_of(date):
        there = date // near
        down = jnp.where(there > place, places - 1 - there, places - 2 - there)
        up = jnp.where(there < place, there, there - 1)
        turn = jnp.where(low, down, up)
        turn = jnp.where(there == place, places - 1, turn)
        return turn * near + lax.rem(date, near)

    barrier = pltpu.get_barrier_semaphore()

    def greet(j, carry):
        @pl.when(j != me)
        def _():
            pl.semaphore_signal(barrier, inc=1, device_id=device(slab, j), device_id_type=MESH)

        @pl.when(has_prior)
        def _():
            pl.semaphore_signal(barrier, inc=1, device_id=device(slab - 1, j), device_id_type=MESH)

        @pl.when(has_next)
        def _():
            pl.semaphore_signal(barrier, inc=1, device_id=device(slab + 1, j), device_id_type=MESH)

        return carry

    def flows_copy(step):
        return pltpu.make_async_copy(
            cashflows.at[date_at(step)], flows.at[step], flows_sem.at[step]
        )

    def state_copy(step):
        return pltpu.make_async_copy(
            factors_far.at[date_at(step)], factors.at[step], state_sem.at[step]
        )

    small = [
        pltpu.make_async_copy(source, target, small_sem.at[i])
        for i, (source, target) in enumerate(
            (
                (frequency_far, frequency),
                (phases_far, phases),
                (margin_lag_far, margin_lag),
                (thresholds_far, thresholds),
                (transfer_min_far, transfer_min),
            )
        )
    ]
    for copy in small:
        copy.start()

    def load(step):
        state_copy(step).start()
        flows_copy(step).start()

    for step in range(min(2 * UNROLL, dates)):
        load(step)
    lax.fori_loop(0, group, greet, 0)

    for copy in small:
        copy.wait()
    turn = split(frequency[...].astype(f32).T * inverse_turn, 3)
    phase = split(as_column(phases[...] * inverse_turn, terms), 3)
    lane = lax.broadcasted_iota(jnp.int32, (terms, risk), 1)
    offset_part = jnp.zeros((terms, risk), f32)
    for i, piece in enumerate(phase):
        offset_part = jnp.where(lane == i, piece.astype(f32)[:, :risk], offset_part)
    wave_map = jnp.concatenate([piece.astype(f32) for piece in turn] + [offset_part], axis=1)
    wave_map = wave_map.astype(bf16)

    def turns_of(source, date, first_column):
        now = source[date, :, pl.ds(first_column, FEATURE_WIDTH)]
        stacked = jnp.concatenate([now, now, now, jnp.ones(now.shape, bf16)], axis=0)
        return contract(wave_map, stacked)

    def wave_of(turns):
        turns = turns - jnp.round(turns)
        square = turns * turns
        total = half_wave[-1]
        for term in half_wave[-2::-1]:
            total = total * square + term
        return (total * total - root_two).astype(bf16)

    def pair_copy(step):
        there = pl.ds(pl.multiple_of((1 - side) * half, 8), half)
        return pltpu.make_async_remote_copy(
            src_ref=partial_sum.at[step, there],
            dst_ref=pair_part.at[step],
            send_sem=pair_send.at[step],
            recv_sem=pair_recv.at[step],
            device_id=device(slab, partner),
            device_id_type=MESH,
        )

    def owner_copy(step, owner, slot):
        return pltpu.make_async_remote_copy(
            src_ref=pair_total.at[step],
            dst_ref=gathered.at[slot],
            send_sem=owner_send.at[step],
            recv_sem=owner_recv.at[slot],
            device_id=device(slab, owner),
            device_id_type=MESH,
        )

    def pair_sum(step):
        here = pl.ds(pl.multiple_of(side * half, 8), half)
        pair_copy(step).wait_recv()
        return partial_sum[step, here] + pair_part[step]

    def deliver(step):
        pair_total[step] = pair_sum(step)
        owner_copy(step, date_at(step) * spread, me).start()

    def deliver_or_keep(step):
        owner = date_at(step) * spread
        total = pair_sum(step)

        @pl.when(owner == me)
        def _():
            gathered[me] = total

        @pl.when(owner != me)
        def _():
            pair_total[step] = total
            owner_copy(step, owner, me).start()

    def prior_copy(target):
        return pltpu.make_async_remote_copy(
            src_ref=factors_far.at[pl.ds(dates - LAG_MAX, LAG_MAX)],
            dst_ref=state,
            send_sem=prior_send,
            recv_sem=prior_recv,
            device_id=device(target, me),
            device_id_type=MESH,
        )

    def gram(steps, done):
        blocks = [(i, c) for i in range(len(steps)) for c in range(0, paths, FEATURE_WIDTH)]
        sums = [None] * len(steps)

        def accumulate(block, now):
            i, column = block
            flow = flows[steps[i], :, pl.ds(column, FEATURE_WIDTH)]
            part = contract_last(jnp.concatenate([now, flow], axis=0), now)
            sums[i] = part if sums[i] is None else sums[i] + part
            if column + FEATURE_WIDTH == paths:
                partial_sum[steps[i]] = sums[i]
                done(i)

        turns = turns_of(factors, steps[0], 0)
        before = None
        for n, (i, column) in enumerate(blocks):
            following = None
            if n + 1 < len(blocks):
                following = turns_of(factors, steps[blocks[n + 1][0]], blocks[n + 1][1])
            if before is not None:
                accumulate(blocks[n - 1], before)
            before = wave_of(turns)
            features[LAG_MAX + steps[i], :, pl.ds(column, FEATURE_WIDTH)] = before
            turns = following
        accumulate(blocks[-1], before)

    def ready(step):
        state_copy(step).wait()
        flows_copy(step).wait()

    def greeted():
        neighbours = (slab + slabs - 1) // slabs + (2 * slabs - 2 - slab) // slabs
        pl.semaphore_wait(barrier, group - 1 + group * neighbours)
        pair_copy(0).start()

        @pl.when(has_next)
        def _():
            prior_copy(slab + 1).start()

    ready(0)
    gram([0], lambda i: greeted())
    for step in range(1, UNROLL):
        ready(step)
        gram([step], lambda i: pair_copy(step).start())

    def forward(turn, carry):
        steps = [UNROLL * turn + i for i in range(UNROLL)]

        @pl.when(turn < dates // UNROLL - 1)
        def _():
            for step in steps:
                load(step + UNROLL)

        for step in steps:
            ready(step)
        deliver(steps[0] - UNROLL)

        def done(i):
            pair_copy(steps[i]).start()
            if i + 1 < UNROLL:
                deliver(steps[i + 1] - UNROLL)

        gram(steps, done)
        return carry

    lax.fori_loop(1, dates // UNROLL, forward, 0)

    for step in range(dates - UNROLL, dates):
        deliver_or_keep(step)

    lag_column[...] = as_column(margin_lag[...].astype(f32), 128)
    offset_column[...] = as_column(
        (thresholds[...] + transfer_min[...]).astype(f32) / 100.0, 128
    )
    totals[...] = jnp.zeros(totals.shape, f32)

    def prior_features(slot):
        @pl.when(has_prior)
        def _():
            if slot == 0:
                prior_copy(slab).wait_recv()
            turns = turns_of(state, slot, 0)
            for column in range(0, paths, FEATURE_WIDTH):
                following = None
                if column + FEATURE_WIDTH < paths:
                    following = turns_of(state, slot, column + FEATURE_WIDTH)
                features[slot, :, pl.ds(column, FEATURE_WIDTH)] = wave_of(turns)
                turns = following

    def coefficients_copy(source, slab_index, path_index, slot, sem):
        return pltpu.make_async_remote_copy(
            src_ref=source,
            dst_ref=coefficients.at[slot],
            send_sem=coefficients_send.at[sem],
            recv_sem=coefficients_recv.at[slot],
            device_id=device(slab_index, path_index),
            device_id_type=MESH,
        )

    own = lax.div(me, spread)
    is_owner = lax.rem(me, spread) == 0
    chips = group // 2
    chip = lax.div(me, 2)
    relay = chips
    onward = chips + dates

    def evaluate(slot, feature_slot):
        for column in range(0, paths, VALUE_WIDTH):
            columns = pl.ds(column, VALUE_WIDTH)
            value = contract(coefficients[slot], features[feature_slot, :, columns])
            values[slot, :, columns] = value.astype(bf16)

    def pass_on(source, date):
        @pl.when(jnp.logical_and(has_next, date >= dates - LAG_MAX))
        def _():
            slot = date - (dates - LAG_MAX)
            coefficients_copy(source, slab + 1, me, slot, onward + slot).start()

    @pl.when(is_owner)
    def _():
        def arrived(j, carry):
            @pl.when(j != me)
            def _():
                owner_copy(0, me, j).wait_recv()

            return carry

        lax.fori_loop(0, group, arrived, 0)
        upper = gathered[0]
        lower = gathered[1]
        for j in range(2, group, 2):
            upper = upper + gathered[j]
            lower = lower + gathered[j + 1]
        sums = jnp.concatenate([upper, lower], axis=0) * (1.0 / paths_all)
        rows = lax.broadcasted_iota(jnp.int32, (terms, terms), 0)
        columns = lax.broadcasted_iota(jnp.int32, (terms, terms), 1)
        system = sums[:terms] + jnp.where(rows == columns, ridge_weight, 0.0)
        answer = solve(system, sums[terms:]).astype(bf16)
        own_coefficients[...] = answer
        coefficients[LAG_MAX + own] = answer

        def tell(turn, carry):
            distance = chips - turn
            for there in (chip + distance, chip - distance):

                @pl.when(jnp.logical_and(there >= 0, there < chips))
                def _():
                    coefficients_copy(
                        own_coefficients, slab, 2 * there + side, LAG_MAX + own, there
                    ).start()

            return carry

        lax.fori_loop(1, chips, tell, 0)
        coefficients_copy(own_coefficients, slab, partner, LAG_MAX + own, chip).start()
        pass_on(own_coefficients, own)
        evaluate(LAG_MAX + own, LAG_MAX + step_of(own))

    def visit(there, which):
        owner = 2 * there + which
        date = lax.div(owner, spread)
        slot = LAG_MAX + date

        @pl.when(jnp.logical_and(lax.rem(owner, spread) == 0, owner != me))
        def _():
            coefficients_copy(own_coefficients, slab, me, slot, 0).wait_recv()

            @pl.when(jnp.logical_and(which == side, there != chip))
            def _():
                coefficients_copy(
                    coefficients.at[slot], slab, partner, slot, relay + date
                ).start()

            pass_on(coefficients.at[slot], date)
            evaluate(slot, LAG_MAX + step_of(date))

    prior_features(0)
    visit(chip, 1 - side)
    for slot in range(1, LAG_MAX):
        prior_features(slot)

    def collect(turn, carry):
        distance = 1 + lax.rem(turn, chips - 1)
        which = lax.rem(side + turn // (chips - 1), 2)

        for there in (chip + distance, chip - distance):

            @pl.when(jnp.logical_and(there >= 0, there < chips))
            def _():
                visit(there, which)

        return carry

    lax.fori_loop(0, 2 * (chips - 1), collect, 0)

    repeat = EXPOSE_WIDTH // 128

    def expose(first_date, end_date):
        lag = jnp.concatenate([lag_column[...]] * repeat, axis=1)
        offset = jnp.concatenate([offset_column[...]] * repeat, axis=1)

        def body(block, carry):
            start = pl.multiple_of(block * EXPOSE_WIDTH, EXPOSE_WIDTH)
            columns = pl.ds(start, EXPOSE_WIDTH)
            earlier = [
                values[first_date + slot, :, columns].astype(f32) for slot in range(LAG_MAX)
            ]
            for date in range(first_date, end_date):
                value = values[LAG_MAX + date, :, columns].astype(f32)
                lagged = jnp.zeros(value.shape, f32)
                for lag_value in range(1, LAG_MAX + 1):
                    lagged = jnp.where(lag == lag_value, earlier[-lag_value], lagged)
                collateral = jnp.maximum(lagged - offset, 0.0)
                open_value = jnp.maximum(value - collateral, 0.0)
                exposure[date, :, columns] = open_value.astype(bf16)
                total = open_value[:, :128]
                for i in range(1, repeat):
                    total = total + open_value[:, 128 * i : 128 * (i + 1)]
                totals[date] = totals[date] + total
                earlier = earlier[1:] + [value]
            return carry

        lax.fori_loop(0, paths // EXPOSE_WIDTH, body, 0)

    expose(LAG_MAX, dates)

    @pl.when(has_prior)
    def _():
        def prior(slot, carry):
            coefficients_copy(own_coefficients, slab, me, slot, 0).wait_recv()
            evaluate(slot, slot)
            return carry

        lax.fori_loop(0, LAG_MAX, prior, 0)

    @pl.when(jnp.logical_not(has_prior))
    def _():
        values[pl.ds(0, LAG_MAX)] = jnp.zeros((LAG_MAX, sets, paths), bf16)

    expose(0, LAG_MAX)
    rows = [jnp.sum(totals[date].T, axis=0, keepdims=True) for date in range(dates)]
    profile_own[...] = jnp.concatenate(rows, axis=0)

    def profile_copy(j, slot):
        return pltpu.make_async_remote_copy(
            src_ref=profile_own,
            dst_ref=profile_all.at[slot],
            send_sem=profile_send.at[j],
            recv_sem=profile_recv.at[slot],
            device_id=device(slab, j),
            device_id_type=MESH,
        )

    def share(j, carry):
        @pl.when(j != me)
        def _():
            profile_copy(j, me).start()

        return carry

    lax.fori_loop(0, group, share, 0)
    profile_all[me] = profile_own[...]

    def received(j, carry):
        @pl.when(j != me)
        def _():
            profile_copy(0, j).wait_recv()

        return carry

    lax.fori_loop(0, group, received, 0)
    total = profile_all[0]
    for j in range(1, group):
        total = total + profile_all[j]
    profile[...] = total * (1.0 / paths_all)

    def sent(step, carry):
        pair_copy(step).wait_send()

        @pl.when(date_at(step) * spread != me)
        def _():
            owner_copy(step, me, me).wait_send()

        return carry

    lax.fori_loop(0, dates, sent, 0)

    def told(j, carry):
        @pl.when(j != me)
        def _():
            profile_copy(j, me).wait_send()

        return carry

    lax.fori_loop(0, group, told, 0)

    @pl.when(is_owner)
    def _():
        def told_chip(there, carry):
            coefficients_copy(own_coefficients, slab, me, 0, there).wait_send()
            return carry

        lax.fori_loop(0, chips, told_chip, 0)

    def relayed(date, carry):
        owner = date * spread

        @pl.when(jnp.logical_and(lax.rem(owner, 2) == side, lax.div(owner, 2) != chip))
        def _():
            coefficients_copy(own_coefficients, slab, me, 0, relay + date).wait_send()

        return carry

    lax.fori_loop(0, dates, relayed, 0)

    @pl.when(has_next)
    def _():
        for slot in range(LAG_MAX):
            coefficients_copy(own_coefficients, slab, me, 0, onward + slot).wait_send()

    @pl.when(has_next)
    def _():
        prior_copy(slab).wait_send()


def local(axes, factors, cashflows, frequency, phases, margin_lag, thresholds, transfer_min):
    slabs, group = axes
    dates, risk, paths = factors.shape
    sets = cashflows.shape[1]
    terms = frequency.shape[0]
    half = (terms + sets) // 2
    anywhere = pl.BlockSpec(memory_space=pltpu.HBM)
    inside = pl.BlockSpec(memory_space=pltpu.VMEM)
    dma = pltpu.SemaphoreType.DMA
    return pl.pallas_call(
        functools.partial(kernel, axes),
        out_shape=(
            pltpu.VMEM(cashflows.shape, bf16),
            jax.ShapeDtypeStruct((dates, sets), f32),
        ),
        in_specs=[anywhere] * 7,
        out_specs=(inside, inside),
        scratch_shapes=[
            pltpu.VMEM((risk, terms), bf16),
            pltpu.VMEM((1, terms), f32),
            pltpu.VMEM((1, sets), jnp.int32),
            pltpu.VMEM((1, sets), jnp.int32),
            pltpu.VMEM((1, sets), jnp.int32),
            pltpu.VMEM((dates, risk, paths), bf16),
            pltpu.VMEM((LAG_MAX, risk, paths), bf16),
            pltpu.VMEM((dates, sets, paths), bf16),
            pltpu.VMEM((LAG_MAX + dates, terms, paths), bf16),
            pltpu.VMEM((dates, terms + sets, terms), f32),
            pltpu.VMEM((dates, half, terms), f32),
            pltpu.VMEM((dates, half, terms), f32),
            pltpu.VMEM((group, half, terms), f32),
            pltpu.VMEM((sets, terms), bf16),
            pltpu.VMEM((LAG_MAX + dates, sets, terms), bf16),
            pltpu.VMEM((dates, sets), f32),
            pltpu.VMEM((group, dates, sets), f32),
            pltpu.VMEM((LAG_MAX + dates, sets, paths), bf16),
            pltpu.VMEM((dates, sets, 128), f32),
            pltpu.VMEM((sets, 128), f32),
            pltpu.VMEM((sets, 128), f32),
            dma((5,)),
            dma((dates,)),
            dma((dates,)),
            dma,
            dma,
            dma((dates,)),
            dma((dates,)),
            dma((dates,)),
            dma((group,)),
            dma((group // 2 + dates + LAG_MAX,)),
            dma((LAG_MAX + dates,)),
            dma((group,)),
            dma((group,)),
        ],
        compiler_params=pltpu.CompilerParams(
            collective_id=0, has_side_effects=True, vmem_limit_bytes=VMEM_LIMIT
        ),
    )(
        factors,
        cashflows,
        frequency.T,
        phases.reshape(1, terms),
        margin_lag.reshape(1, sets),
        thresholds.reshape(1, sets),
        transfer_min.reshape(1, sets),
    )


def solution(mesh):
    axes = (mesh.shape["date"], mesh.shape["path"])
    return jax.shard_map(
        functools.partial(local, axes),
        mesh=mesh,
        in_specs=(P("date", None, "path"), P("date", None, "path"), P(), P(), P(), P(), P()),
        out_specs=(P("date", None, "path"), P("date", None)),
        check_vma=False,
    )
```
